32 devices in a mesh: section: 2 (over core), fsdp: 4 (over y, x), tp: 4 (over z).
Axes of the slice: x: 2, y: 2, z: 4, core: 2. Of those that a mesh axis runs over, the one named last changes fastest.
Arguments:
- saved_inputs: bfloat16 [2, 8, 256, 2560], P('section', None, 'fsdp', 'tp'), may hold values from -6 to 6
- top_grad: bfloat16 [8, 256, 2560], P(None, 'fsdp', 'tp'), may hold values from -6 to 6
- norm_gain: float32 [2, 2560], P('section'), may hold values from 0.5 to 1.5
- gate_weight: bfloat16 [2, 2560, 6912], P('section', 'fsdp', 'tp'), may hold values from -0.125 to 0.125
- up_weight: bfloat16 [2, 2560, 6912], P('section', 'fsdp', 'tp'), may hold values from -0.125 to 0.125
- down_weight: bfloat16 [2, 6912, 2560], P('section', 'tp', 'fsdp'), may hold values from -0.078125 to 0.078125
Outputs:
- input_grads: bfloat16 [2, 8, 256, 2560], P('section', None, 'fsdp', 'tp')
- gate_grad: float32 [2, 2560, 6912], P('section', 'fsdp', 'tp')
- up_grad: float32 [2, 2560, 6912], P('section', 'fsdp', 'tp')
- down_grad: float32 [2, 6912, 2560], P('section', 'tp', 'fsdp')
- gain_grad: float32 [2, 2560], P('section', 'tp')
The draws below stay inside these ranges and needn't reach their ends.
All inputs are finite; a program needn't handle non-finite values.
Results may differ from the reference program's by a relative error of at most 0.0055.
Values may be sent and summed in bfloat16 or wider, within the bound.
A program may use at most 192 MiB of HBM per device.

```python
import jax
import jax.numpy as jnp
from jax import lax

D = 2560
FF = 6912
MICRO = 8
SECTIONS = 2
TOKENS = 256


def block_levels(key, shape, pieces, least, high):
    factor_of = 1.0
    for position, shards_of in pieces:
        steps = jax.random.uniform(jax.random.fold_in(jax.random.fold_in(key, 6), position), (shards_of,), jnp.float32, least / len(pieces), high / len(pieces))
        factor_of = factor_of * jnp.repeat(jnp.exp(steps), shape[position] // shards_of).reshape((-1,) + (1,) * (len(shape) - 1 - position))
    return factor_of


def scatter_about(rng, dims, width, limit, cuts=(), kind=jnp.bfloat16):
    factor_of = block_levels(rng, dims, cuts, -0.22, 0.18) if cuts else 1.0
    drawn = jax.random.normal(rng, dims, jnp.float32) * width * factor_of
    return jnp.minimum(jnp.maximum(drawn, -limit), limit).astype(kind)


def setup_inputs(seed: int = 0) -> dict:
    streams_of = jax.random.split(jax.random.key(seed), 7)
    saved_inputs = scatter_about(streams_of[0], (SECTIONS, MICRO, TOKENS, D), 1.0, 6.0, ((0, 2), (2, 4), (3, 4)))
    top_grad = scatter_about(streams_of[1], (MICRO, TOKENS, D), 1.0, 6.0, ((1, 4), (2, 4)))
    norm_gain = jnp.clip(1.0 + 0.1 * jax.random.normal(streams_of[2], (SECTIONS, D), jnp.float32), 0.5, 1.5)
    gate_weight = scatter_about(streams_of[3], (SECTIONS, D, FF), D ** -0.5, 0.125, ((0, 2), (1, 4), (2, 4)))
    up_weight = scatter_about(streams_of[4], (SECTIONS, D, FF), D ** -0.5, 0.125, ((0, 2), (1, 4), (2, 4)))
    down_weight = scatter_about(streams_of[5], (SECTIONS, FF, D), FF ** -0.5, 0.078125, ((0, 2), (1, 4), (2, 4)))
    return {"saved_inputs": saved_inputs, "top_grad": top_grad, "norm_gain": norm_gain, "gate_weight": gate_weight, "up_weight": up_weight, "down_weight": down_weight}


epsilon = 1e-05

def layer_backward(inputs, cotangent, gain_row, w_gate, w_up, w_down):
    inputs_wide = inputs.astype(jnp.float32)
    row_scale = lax.rsqrt(lax.optimization_barrier(jnp.mean(inputs_wide * inputs_wide, axis=-1, keepdims=True)) + epsilon)
    unit_rows = inputs_wide * row_scale
    normed = (unit_rows * gain_row).astype(jnp.bfloat16)
    gate_pre = jnp.dot(normed, w_gate, preferred_element_type=jnp.float32)
    upward = jnp.dot(normed, w_up, preferred_element_type=jnp.float32)
    gate_sigmoid = jax.nn.sigmoid(gate_pre)
    silu_out = gate_pre * gate_sigmoid
    hidden = (silu_out * upward).astype(jnp.bfloat16)
    d_hidden = jnp.dot(cotangent, w_down.T, preferred_element_type=jnp.float32)
    d_gate = (d_hidden * upward * gate_sigmoid * (1.0 + gate_pre * (1.0 - gate_sigmoid))).astype(jnp.bfloat16)
    d_up = (d_hidden * silu_out).astype(jnp.bfloat16)
    d_normed = jnp.dot(d_gate, w_gate.T, preferred_element_type=jnp.float32) + jnp.dot(d_up, w_up.T, preferred_element_type=jnp.float32)
    scaled = d_normed * gain_row
    norm_stat = lax.optimization_barrier(jnp.mean(scaled * unit_rows, axis=-1, keepdims=True))
    d_inputs = (cotangent.astype(jnp.float32) + row_scale * (scaled - unit_rows * norm_stat)).astype(jnp.bfloat16)
    gate_term = jnp.dot(normed.T, d_gate, preferred_element_type=jnp.float32)
    up_term = jnp.dot(normed.T, d_up, preferred_element_type=jnp.float32)
    down_term = jnp.dot(hidden.T, cotangent, preferred_element_type=jnp.float32)
    gain_term = lax.optimization_barrier(jnp.sum(d_normed * unit_rows, axis=0))
    return (d_inputs, (gate_term, up_term, down_term, gain_term))

def reference(saved_inputs, top_grad, norm_gain, gate_weight, up_weight, down_weight):
    incoming = top_grad
    per_section = []
    for section_number in range(SECTIONS - 1, -1, -1):

        def one_micro(totals, paired):
            d_inputs, gradients = layer_backward(paired[0], paired[1], norm_gain[section_number], gate_weight[section_number], up_weight[section_number], down_weight[section_number])
            summed = (totals[0] + gradients[0], totals[1] + gradients[1], totals[2] + gradients[2], totals[3] + gradients[3])
            return (summed, d_inputs)
        zeros_init = (jnp.zeros((D, FF), jnp.float32), jnp.zeros((D, FF), jnp.float32), jnp.zeros((FF, D), jnp.float32), jnp.zeros((D,), jnp.float32))
        totals, incoming = lax.scan(one_micro, zeros_init, (saved_inputs[section_number], incoming))
        per_section.append((incoming, totals[0], totals[1], totals[2], totals[3]))
    ordered = per_section[::-1]
    input_grads = jnp.stack([item[0] for item in ordered])
    gate_grad = jnp.stack([item[1] for item in ordered])
    up_grad = jnp.stack([item[2] for item in ordered])
    down_grad = jnp.stack([item[3] for item in ordered])
    gain_grad = jnp.stack([item[4] for item in ordered])
    return (input_grads, gate_grad, up_grad, down_grad, gain_grad)
```

```python
import math

import jax
import jax.numpy as jnp
from jax import lax
from jax.sharding import PartitionSpec as P

epsilon = 1e-05
GROUPS = 2


def contract_rows(left, right):
    return lax.dot_general(
        left, right, (((0,), (0,)), ((), ())), preferred_element_type=jnp.float32
    )


def contract_cols(left, right):
    return lax.dot_general(
        left, right, (((1,), (1,)), ((), ())), preferred_element_type=jnp.float32
    )


def shifted(block, axis, shift):
    count = lax.axis_size(axis)
    return lax.ppermute(block, axis, [(i, (i + shift) % count) for i in range(count)])


def gather_columns(block, axis):
    count = lax.axis_size(axis)
    index = lax.axis_index(axis)
    rows, width = block.shape
    pieces = [block] + [shifted(block, axis, k) for k in range(1, count)]
    whole = jnp.zeros((rows, width * count), block.dtype)
    for k, piece in enumerate(pieces):
        source = lax.rem(index - k + count, count)
        whole = lax.dynamic_update_slice(whole, piece, (0, source * width))
    return whole


def swap_columns(block, axis):
    count = lax.axis_size(axis)
    index = lax.axis_index(axis)
    rows = block.shape[0]
    width = block.shape[1] // count
    whole = jnp.zeros((rows * count, width), block.dtype)
    for k in range(count):
        target = lax.rem(index + k, count)
        piece = lax.dynamic_slice_in_dim(block, target * width, width, 1)
        if k:
            piece = shifted(piece, axis, k)
        source = lax.rem(index - k + count, count)
        whole = lax.dynamic_update_slice(whole, piece, (source * rows, 0))
    return whole


def sum_columns(partial, axis):
    count = lax.axis_size(axis)
    index = lax.axis_index(axis)
    width = partial.shape[1] // count
    short = partial.astype(jnp.bfloat16)
    total = lax.dynamic_slice_in_dim(partial, index * width, width, 1)
    for k in range(1, count):
        target = lax.rem(index + k, count)
        piece = lax.dynamic_slice_in_dim(short, target * width, width, 1)
        total = total + shifted(piece, axis, k).astype(jnp.float32)
    return total


def sum_all(value, axis):
    total = value
    for k in range(1, lax.axis_size(axis)):
        total = total + shifted(value, axis, k)
    return total


def shards(saved_inputs, top_grad, norm_gain, gate_weight, up_weight, down_weight):
    section_count = lax.axis_size("section")
    section_index = lax.axis_index("section")
    fsdp_count = lax.axis_size("fsdp")
    micro_count, row_count, local_width = saved_inputs.shape[1:]
    groups = math.gcd(GROUPS, micro_count)
    rows = micro_count // groups * row_count
    full_width = local_width * lax.axis_size("tp")
    hidden_width = gate_weight.shape[2]
    slice_width = down_weight.shape[2]

    w_gate = lax.all_gather(gate_weight[0], "fsdp", axis=0, tiled=True)
    w_up = lax.all_gather(up_weight[0], "fsdp", axis=0, tiled=True)
    w_down = lax.all_gather(down_weight[0], "fsdp", axis=0, tiled=True)

    gain_full = norm_gain[0]
    column_start = lax.axis_index("tp") * local_width
    gain_local = lax.dynamic_slice_in_dim(gain_full, column_start, local_width)

    x_local = saved_inputs[0].reshape(micro_count * row_count, local_width)
    x_full = gather_columns(x_local, "tp")
    top_local = top_grad.reshape(micro_count * row_count, local_width)
    top_full = gather_columns(top_local, "tp")
    x_wide = x_full.astype(jnp.float32)
    row_scale = lax.rsqrt(jnp.mean(x_wide * x_wide, axis=-1, keepdims=True) + epsilon)
    normed = (x_wide * row_scale * gain_full).astype(jnp.bfloat16)
    spans = [slice(g * rows, (g + 1) * rows) for g in range(groups)]
    normed_swapped = [swap_columns(normed[span], "fsdp") for span in spans]
    gate_pre = jnp.dot(normed, w_gate, preferred_element_type=jnp.float32)
    upward = jnp.dot(normed, w_up, preferred_element_type=jnp.float32)
    gate_sigmoid = jax.nn.sigmoid(gate_pre)
    hidden = (gate_pre * gate_sigmoid * upward).astype(jnp.bfloat16)
    hidden_all = [lax.all_gather(hidden[span], "fsdp", axis=0, tiled=True) for span in spans]
    last_section = section_index == section_count - 1

    def of_group(array, group):
        return lax.dynamic_slice_in_dim(array, group * rows, rows, 0)

    ticks = []
    received = jnp.zeros((rows, local_width), jnp.bfloat16)
    totals = [None, None, None]
    grads = []
    gain_total = jnp.zeros((local_width,), jnp.float32)

    def own(items, group):
        chosen = items[group]
        for s in range(section_count - 1):
            chosen = jnp.where(section_index == s, items[group + section_count - 1 - s], chosen)
        return chosen

    for tick in range(groups + section_count - 1):
        raw = tick - (section_count - 1 - section_index)
        valid = (raw >= 0) & (raw < groups)
        group = jnp.clip(raw, 0, groups - 1)
        top_group = min(tick, groups - 1)
        from_top = top_local[top_group * rows : (top_group + 1) * rows]
        cotangent = jnp.where(last_section, from_top, received)
        full_top = top_full[top_group * rows : (top_group + 1) * rows]
        if tick == 0:
            full_cotangent = full_top
        else:
            full_cotangent = jnp.where(last_section, full_top, gather_columns(received, "tp"))

        gate_now = of_group(gate_pre, group)
        up_now = of_group(upward, group)
        sigmoid_now = jax.nn.sigmoid(gate_now)
        d_hidden = contract_cols(full_cotangent[:, :slice_width], w_down[:hidden_width])
        for k in range(1, fsdp_count):
            d_hidden = d_hidden + contract_cols(
                full_cotangent[:, k * slice_width : (k + 1) * slice_width],
                w_down[k * hidden_width : (k + 1) * hidden_width],
            )
        d_gate = (
            d_hidden * up_now * sigmoid_now * (1.0 + gate_now * (1.0 - sigmoid_now))
        ).astype(jnp.bfloat16)
        d_up = (d_hidden * (gate_now * sigmoid_now)).astype(jnp.bfloat16)
        ticks.append((d_gate, d_up, full_cotangent))

        partial = contract_cols(d_gate, w_gate) + contract_cols(d_up, w_up)
        scale_now = of_group(row_scale, group)
        unit_full = of_group(x_full, group).astype(jnp.float32) * scale_now
        stat = jnp.sum(partial * gain_full * unit_full, axis=-1)
        norm_stat = (sum_all(stat, "tp") / full_width)[:, None]
        d_normed = sum_columns(partial, "tp")
        unit_local = of_group(x_local, group).astype(jnp.float32) * scale_now
        d_inputs = (
            cotangent.astype(jnp.float32)
            + scale_now * (d_normed * gain_local - unit_local * norm_stat)
        ).astype(jnp.bfloat16)
        gain_total = gain_total + jnp.where(valid, jnp.sum(d_normed * unit_local, axis=0), 0.0)
        grads.append(d_inputs)
        if tick < groups + section_count - 2:
            received = lax.ppermute(
                d_inputs, "section", [(s, s - 1) for s in range(1, section_count)]
            )

        done = tick - (section_count - 1)
        if done >= 0:
            gates, ups, cotangents = zip(*ticks)
            both = jnp.concatenate([own(gates, done), own(ups, done)], axis=1)
            both = lax.all_gather(both, "fsdp", axis=0, tiled=True)
            swapped = swap_columns(own(cotangents, done), "fsdp")
            terms = (
                contract_rows(normed_swapped[done], both[:, :hidden_width]),
                contract_rows(normed_swapped[done], both[:, hidden_width:]),
                contract_rows(hidden_all[done], swapped),
            )
            totals = [b if a is None else a + b for a, b in zip(totals, terms)]

    out = jnp.concatenate([own(grads, g) for g in range(groups)], axis=0)
    out = out.reshape(micro_count, row_count, local_width)
    gain_share = lax.psum(gain_total, "fsdp")
    return (out[None], totals[0][None], totals[1][None], totals[2][None], gain_share[None])


def solution(mesh):
    placed = (
        P("section", None, "fsdp", "tp"),
        P(None, "fsdp", "tp"),
        P("section", None),
        P("section", "fsdp", "tp"),
        P("section", "fsdp", "tp"),
        P("section", "tp", "fsdp"),
    )
    return jax.shard_map(
        shards,
        mesh=mesh,
        in_specs=placed,
        out_specs=(
            P("section", None, "fsdp", "tp"),
            P("section", "fsdp", "tp"),
            P("section", "fsdp", "tp"),
            P("section", "tp", "fsdp"),
            P("section", "tp"),
        ),
        check_vma=False,
    )
```

```python
import math

import jax
import jax.numpy as jnp
from jax import lax
from jax.sharding import PartitionSpec as P

epsilon = 1e-05
GROUPS = 2


def contract_rows(left, right):
    return lax.dot_general(
        left, right, (((0,), (0,)), ((), ())), preferred_element_type=jnp.float32
    )


def contract_cols(left, right):
    return lax.dot_general(
        left, right, (((1,), (1,)), ((), ())), preferred_element_type=jnp.float32
    )


def shifted(block, axis, shift):
    count = lax.axis_size(axis)
    return lax.ppermute(block, axis, [(i, (i + shift) % count) for i in range(count)])


def gather_columns(block, axis):
    count = lax.axis_size(axis)
    index = lax.axis_index(axis)
    rows, width = block.shape
    pieces = [block] + [shifted(block, axis, k) for k in range(1, count)]
    whole = jnp.zeros((rows, width * count), block.dtype)
    for k, piece in enumerate(pieces):
        source = lax.rem(index - k + count, count)
        whole = lax.dynamic_update_slice(whole, piece, (0, source * width))
    return whole


def swap_columns(block, axis, whole, group, groups):
    count = lax.axis_size(axis)
    index = lax.axis_index(axis)
    rows = block.shape[0]
    width = block.shape[1] // count
    for k in range(count):
        target = lax.rem(index + k, count)
        piece = lax.dynamic_slice_in_dim(block, target * width, width, 1)
        if k:
            piece = shifted(piece, axis, k)
        source = lax.rem(index - k + count, count)
        whole = lax.dynamic_update_slice(whole, piece, ((source * groups + group) * rows, 0))
    return whole


def sum_columns(partial, axis):
    count = lax.axis_size(axis)
    index = lax.axis_index(axis)
    width = partial.shape[1] // count
    short = partial.astype(jnp.bfloat16)
    total = lax.dynamic_slice_in_dim(partial, index * width, width, 1)
    for k in range(1, count):
        target = lax.rem(index + k, count)
        piece = lax.dynamic_slice_in_dim(short, target * width, width, 1)
        total = total + shifted(piece, axis, k).astype(jnp.float32)
    return total


def sum_all(value, axis):
    total = value
    for k in range(1, lax.axis_size(axis)):
        total = total + shifted(value, axis, k)
    return total


def shards(saved_inputs, top_grad, norm_gain, gate_weight, up_weight, down_weight):
    section_count = lax.axis_size("section")
    section_index = lax.axis_index("section")
    fsdp_count = lax.axis_size("fsdp")
    micro_count, row_count, local_width = saved_inputs.shape[1:]
    groups = math.gcd(GROUPS, micro_count)
    rows = micro_count // groups * row_count
    full_width = local_width * lax.axis_size("tp")
    hidden_width = gate_weight.shape[2]
    slice_width = down_weight.shape[2]

    w_gate = lax.all_gather(gate_weight[0], "fsdp", axis=0, tiled=True)

    gain_full = norm_gain[0]
    column_start = lax.axis_index("tp") * local_width
    gain_local = lax.dynamic_slice_in_dim(gain_full, column_start, local_width)

    x_local = saved_inputs[0].reshape(micro_count * row_count, local_width)
    x_full = gather_columns(x_local, "tp")
    top_local = top_grad.reshape(micro_count * row_count, local_width)
    top_full = gather_columns(top_local, "tp")
    x_wide = x_full.astype(jnp.float32)
    row_scale = lax.rsqrt(jnp.mean(x_wide * x_wide, axis=-1, keepdims=True) + epsilon)
    normed = (x_wide * row_scale * gain_full).astype(jnp.bfloat16)
    spans = [slice(g * rows, (g + 1) * rows) for g in range(groups)]
    w_up = lax.all_gather(up_weight[0], "fsdp", axis=0, tiled=True)
    blank = jnp.zeros((fsdp_count * rows, slice_width), jnp.bfloat16)
    normed_swapped = [swap_columns(normed[span], "fsdp", blank, 0, 1) for span in spans]
    top_full, normed_swapped, w_gate, w_up, down_local = lax.optimization_barrier(
        (top_full, normed_swapped, w_gate, w_up, down_weight[0])
    )
    w_down = lax.all_gather(down_local, "fsdp", axis=0, tiled=True)
    cotangent_swapped = jnp.zeros((fsdp_count * groups * rows, slice_width), jnp.bfloat16)
    gate_pre = jnp.dot(normed, w_gate, preferred_element_type=jnp.float32)
    upward = jnp.dot(normed, w_up, preferred_element_type=jnp.float32)
    gate_sigmoid = jax.nn.sigmoid(gate_pre)
    hidden = (gate_pre * gate_sigmoid * upward).astype(jnp.bfloat16)
    hidden, gate_pre, upward, w_down = lax.optimization_barrier((hidden, gate_pre, upward, w_down))
    hidden_all = lax.all_gather(hidden, "fsdp", axis=0, tiled=True)
    gathered = hidden_all
    last_section = section_index == section_count - 1

    def of_group(array, group):
        return lax.dynamic_slice_in_dim(array, group * rows, rows, 0)

    ticks = []
    received = jnp.zeros((rows, local_width), jnp.bfloat16)
    totals = [None, None]
    grads = []
    gain_total = jnp.zeros((local_width,), jnp.float32)

    def own(items, group):
        chosen = items[group]
        for s in range(section_count - 1):
            chosen = jnp.where(section_index == s, items[group + section_count - 1 - s], chosen)
        return chosen

    def added(sums, item):
        tokens, both = item
        terms = (
            contract_rows(tokens, both[:, :hidden_width]),
            contract_rows(tokens, both[:, hidden_width:]),
        )
        return [b if a is None else a + b for a, b in zip(sums, terms)]

    for tick in range(groups + section_count - 1):
        raw = tick - (section_count - 1 - section_index)
        valid = (raw >= 0) & (raw < groups)
        group = jnp.clip(raw, 0, groups - 1)
        top_group = min(tick, groups - 1)
        from_top = top_local[top_group * rows : (top_group + 1) * rows]
        cotangent = jnp.where(last_section, from_top, received)
        full_top = top_full[top_group * rows : (top_group + 1) * rows]
        if tick == 0:
            full_cotangent = full_top
        else:
            full_cotangent = jnp.where(last_section, full_top, gather_columns(received, "tp"))

        gate_now = of_group(gate_pre, group)
        up_now = of_group(upward, group)
        sigmoid_now = jax.nn.sigmoid(gate_now)
        d_hidden = contract_cols(full_cotangent[:, :slice_width], w_down[:hidden_width])
        for k in range(1, fsdp_count):
            d_hidden = d_hidden + contract_cols(
                full_cotangent[:, k * slice_width : (k + 1) * slice_width],
                w_down[k * hidden_width : (k + 1) * hidden_width],
            )
        d_gate = (
            d_hidden * up_now * sigmoid_now * (1.0 + gate_now * (1.0 - sigmoid_now))
        ).astype(jnp.bfloat16)
        d_up = (d_hidden * (gate_now * sigmoid_now)).astype(jnp.bfloat16)
        ticks.append((d_gate, d_up, full_cotangent))
        done = tick - (section_count - 1)
        if done >= 0:
            gates, ups, cotangents = zip(*ticks)
            both = jnp.concatenate([own(gates, done), own(ups, done)], axis=1)
            both, d_gate, d_up, gathered = lax.optimization_barrier((both, d_gate, d_up, gathered))
            if done == 0:
                hidden_all = gathered
            both = gathered = lax.all_gather(both, "fsdp", axis=0, tiled=True)
            cotangent_swapped = swap_columns(
                own(cotangents, done), "fsdp", cotangent_swapped, done, groups
            )
            pending = (normed_swapped[done], both)

        partial = contract_cols(d_gate, w_gate) + contract_cols(d_up, w_up)
        scale_now = of_group(row_scale, group)
        unit_full = of_group(x_full, group).astype(jnp.float32) * scale_now
        stat = jnp.sum(partial * gain_full * unit_full, axis=-1)
        norm_stat = (sum_all(stat, "tp") / full_width)[:, None]
        d_normed = sum_columns(partial, "tp")
        if done > 0:
            totals = added(totals, earlier)
        if done >= 0:
            earlier = pending
        unit_local = of_group(x_local, group).astype(jnp.float32) * scale_now
        d_inputs = (
            cotangent.astype(jnp.float32)
            + scale_now * (d_normed * gain_local - unit_local * norm_stat)
        ).astype(jnp.bfloat16)
        gain_total = gain_total + jnp.where(valid, jnp.sum(d_normed * unit_local, axis=0), 0.0)
        grads.append(d_inputs)
        if tick < groups + section_count - 2:
            received = lax.ppermute(
                d_inputs, "section", [(s, s - 1) for s in range(1, section_count)]
            )

    out = jnp.concatenate([own(grads, g) for g in range(groups)], axis=0)
    out = out.reshape(micro_count, row_count, local_width)
    gain_share = jnp.sum(gather_columns(gain_total[None], "fsdp").reshape(fsdp_count, local_width), axis=0)
    totals = added(totals, earlier)
    down_total = contract_rows(hidden_all, cotangent_swapped)
    return (out[None], totals[0][None], totals[1][None], down_total[None], gain_share[None])


def solution(mesh):
    placed = (
        P("section", None, "fsdp", "tp"),
        P(None, "fsdp", "tp"),
        P("section", None),
        P("section", "fsdp", "tp"),
        P("section", "fsdp", "tp"),
        P("section", "tp", "fsdp"),
    )
    return jax.shard_map(
        shards,
        mesh=mesh,
        in_specs=placed,
        out_specs=(
            P("section", None, "fsdp", "tp"),
            P("section", "fsdp", "tp"),
            P("section", "fsdp", "tp"),
            P("section", "tp", "fsdp"),
            P("section", "tp"),
        ),
        check_vma=False,
    )
```
